32 devices in a mesh: block: 2 (over z_hi), span: 4 (over y, x), group: 4 (over z_lo, core).
Axes of the slice: x: 2, y: 2, z: 4 (z_hi: 2, z_lo: 2; z = z_hi * 2 + z_lo), core: 2. Of those that a mesh axis runs over, the one named last changes fastest.
Arguments:
- key_rows: bfloat16 [8, 12288, 8, 128], P(None, ('block', 'span'), 'group'), may hold values from -6 to 6
- value_rows: bfloat16 [8, 12288, 8, 128], P(None, ('block', 'span'), 'group'), may hold values from -6 to 6
- turn_angle: float32 [12288, 64], replicated, may hold values from -3.140625 to 3.140625
- key_gain: float32 [128], replicated, may hold values from 0.25 to 1.75
Outputs:
- stored_keys: bfloat16 [8, 8, 128, 12288], P(('block', 'span'), 'group')
- stored_values: bfloat16 [8, 12288, 8, 128], P(('block', 'span'), None, 'group')
- key_scale: float32 [8, 8, 128], P(('block', 'span'), 'group')
The draws below stay inside these ranges and needn't reach their ends.
All inputs are finite; a program needn't handle non-finite values. Where the reference program divides by a largest or mean magnitude, that divisor is 1e-20 or more.
Results may differ from the reference program's by a relative error of at most 0.001.
Values may be sent and summed in bfloat16 or wider, within the bound.
A program may use at most 128 MiB of HBM per device.

```python
import jax
import jax.numpy as jnp
from jax import lax

BATCH = 8
LENGTH = 12288
KV_HEADS = 8
HEAD_SIZE = 128
HALF_HEAD = 64


def shard_levels(key, dims, pieces, smallest, largest):
    factor_of = 1.0
    for axis_at, parts in pieces:
        heights = jax.random.uniform(jax.random.fold_in(jax.random.fold_in(key, 6), axis_at), (parts,), jnp.float32, smallest / len(pieces), largest / len(pieces))
        factor_of = factor_of * jnp.repeat(jnp.exp(heights), dims[axis_at] // parts).reshape((-1,) + (1,) * (len(dims) - 1 - axis_at))
    return factor_of


def gaussian(rng, extent, spread, reach, split=(), dtype=jnp.bfloat16):
    factor_of = shard_levels(rng, extent, split, -0.22, 0.18) if split else 1.0
    array = jax.random.normal(rng, extent, jnp.float32) * spread * factor_of
    return jnp.minimum(jnp.maximum(array, -reach), reach).astype(dtype)


def setup_inputs(seed: int = 0) -> dict:
    key_list = jax.random.split(jax.random.key(seed), 5)
    key_rows = gaussian(key_list[0], (BATCH, LENGTH, KV_HEADS, HEAD_SIZE), 1.0, 6.0, ((1, 8), (2, 4)))
    value_rows = gaussian(key_list[1], (BATCH, LENGTH, KV_HEADS, HEAD_SIZE), 1.0, 6.0, ((1, 8), (2, 4)))
    turn_angle = jnp.clip(jax.random.uniform(key_list[2], (LENGTH, HALF_HEAD), jnp.float32, -3.140625, 3.140625), -3.140625, 3.140625)
    key_gain = jnp.clip(1.0 + 0.15 * jax.random.normal(key_list[3], (HEAD_SIZE,), jnp.float32), 0.25, 1.75)
    return dict(key_rows=key_rows, value_rows=value_rows, turn_angle=turn_angle, key_gain=key_gain)


def apply_rotary(vectors, angle):
    half = vectors.shape[-1] // 2
    cosine, sine = (jnp.cos(angle)[None, :, None, :], jnp.sin(angle)[None, :, None, :])
    first, second = (vectors[..., :half], vectors[..., half:])
    return jnp.concatenate([first * cosine - second * sine, second * cosine + first * sine], axis=-1)

def unit_rows(vectors, row_gain):
    return vectors * lax.rsqrt(lax.optimization_barrier(jnp.mean(vectors * vectors, axis=-1, keepdims=True)) + 1e-06) * row_gain

def ready_to_store(plain_keys, angle, key_gain):
    wide_keys = plain_keys.astype(jnp.float32)
    wide_keys = unit_rows(wide_keys, key_gain)
    return apply_rotary(wide_keys, angle)

def reference(key_rows, value_rows, turn_angle, key_gain):
    turned_keys = ready_to_store(key_rows, turn_angle, key_gain)
    key_scale = lax.optimization_barrier(jnp.max(jnp.abs(turned_keys), axis=1))
    narrow_keys = (turned_keys / key_scale[:, None]).astype(jnp.bfloat16)
    stored_keys = jnp.transpose(narrow_keys, (0, 2, 3, 1))
    stored_values = value_rows
    return (stored_keys, stored_values, key_scale)
```

```python
import functools

import jax
import jax.numpy as jnp
from jax import lax
from jax.experimental import pallas as pl
from jax.experimental.pallas import tpu as pltpu
from jax.sharding import PartitionSpec as P

MESH = pl.DeviceIdType.MESH
ANY = pltpu.MemorySpace.HBM
TILE = 128
EPS = 1e-06


def flip(index, offset, size):
    out, width = 0, 1
    while width < size:
        out = out + ((index // width) % 2 + (offset // width) % 2) % 2 * width
        width *= 2
    return out


def sin_cos(angle):
    h = angle * 0.5
    q = h * h
    s = 1.0 / 6227020800.0
    for c in (-1.0 / 39916800, 1.0 / 362880, -1.0 / 5040, 1.0 / 120, -1.0 / 6, 1.0):
        s = s * q + c
    s = s * h
    k = -1.0 / 87178291200.0
    for c in (1.0 / 479001600, -1.0 / 3628800, 1.0 / 40320, -1.0 / 720, 1.0 / 24, -0.5, 1.0):
        k = k * q + c
    return 2.0 * s * k, 1.0 - 2.0 * s * s


def exchange(
    nb, ns, ng, heads,
    key_ref, value_ref, angle_ref, gain_ref,
    okey_ref, ovalue_ref, scale_ref,
    kbuf, relay, turned, angles, gains, peak, wide, own,
    send_sem, recv_sem, hop_send, hop_recv, fwd_send, fwd_recv, local_sem,
):
    n, rows = key_ref.shape[0], key_ref.shape[1]
    places = rows // heads
    half = (rows // 2) // (TILE * heads) * (TILE * heads)
    rest = rows - half
    size = wide.shape[1]
    mid = size // 2
    b, s, g = (lax.axis_index(a) for a in ("block", "span", "group"))
    me = b * ns + s
    low = ng // 2
    line = b * 2 + g // low

    def peer(d, b=b, s=s):
        return (b + d // ns) % nb, flip(s, d % ns, ns)

    def shifted(step):
        at = (line + step) % (2 * nb)
        return at // 2, (at % 2) * low + g % low

    down, up = shifted(2 * nb - 1), shifted(1)
    far = [d for d in range(ns, n)]
    near = [d for d in range(1, ns)]

    bar = pltpu.get_barrier_semaphore()
    for d in near + far:
        pb, ps = peer(d)
        pl.semaphore_signal(bar, inc=1, device_id=(pb, ps, g), device_id_type=MESH)
    for e in range(ns):
        pl.semaphore_signal(bar, inc=1, device_id=(up[0], flip(s, e, ns), up[1]), device_id_type=MESH)
    pl.semaphore_wait(bar, n - 1 + ns)

    sources = (key_ref, value_ref)
    sinks = (kbuf, ovalue_ref)

    def direct(a, d):
        pb, ps = peer(d)
        r = pb * ns + ps
        part = pl.ds(0, rows) if d < ns else pl.ds(0, half)
        return pltpu.make_async_remote_copy(
            src_ref=sources[a].at[r, part], dst_ref=sinks[a].at[me, part],
            send_sem=send_sem.at[a, d], recv_sem=recv_sem.at[a, d],
            device_id=(pb, ps, g), device_id_type=MESH,
        )

    def hop(a, d):
        pb, ps = peer(d)
        r = pb * ns + ps
        return pltpu.make_async_remote_copy(
            src_ref=sources[a].at[r, pl.ds(half, rest)], dst_ref=relay.at[a, d - ns],
            send_sem=hop_send.at[a, d], recv_sem=hop_recv.at[a, d],
            device_id=(down[0], s, down[1]), device_id_type=MESH,
        )

    def forward(a, d):
        owner = up[0] * ns + s
        pb, ps = peer(d, up[0], s)
        return pltpu.make_async_remote_copy(
            src_ref=relay.at[a, d - ns], dst_ref=sinks[a].at[owner, pl.ds(half, rest)],
            send_sem=fwd_send.at[a, d], recv_sem=fwd_recv.at[a, d],
            device_id=(pb, ps, up[1]), device_id_type=MESH,
        )

    for d in far:
        hop(0, d).start()
    order = []
    for i in range(max(len(near), len(far))):
        order += far[i:i + 1] + near[i:i + 1]
    for d in order:
        direct(0, d).start()
    load_angle = pltpu.make_async_copy(angle_ref, angles, local_sem.at[0])
    load_angle.start()
    load_key = pltpu.make_async_copy(key_ref.at[me], kbuf.at[me], local_sem.at[1])
    load_key.start()
    load_value = pltpu.make_async_copy(value_ref.at[me], own, local_sem.at[2])
    load_value.start()
    for d in order:
        direct(1, d).start()

    gains[...] = jnp.broadcast_to(gain_ref[...], (size, size)).T
    peak[...] = jnp.zeros_like(peak)

    def turn(r, first, count):
        def tile(i, carry):
            at = first + i * TILE
            wide[...] = kbuf[r, pl.ds(pl.multiple_of(at * heads, TILE * heads), TILE * heads), :].astype(jnp.float32)
            cols = pl.ds(pl.multiple_of(r * places + at, TILE), TILE)
            sine, cosine = sin_cos(angles[:, cols])
            for h in range(heads):
                x = wide[pl.ds(h, TILE, stride=heads), :].T
                norm = lax.rsqrt(jnp.mean(x * x, axis=0, keepdims=True) + EPS)
                x = x * norm * gains[...]
                lo, hi = x[:mid], x[mid:]
                lo, hi = lo * cosine - hi * sine, hi * cosine + lo * sine
                turned[h, :mid, cols] = lo
                turned[h, mid:, cols] = hi
                peak[h, :mid] = jnp.maximum(peak[h, :mid], jnp.abs(lo))
                peak[h, mid:] = jnp.maximum(peak[h, mid:], jnp.abs(hi))
            return carry

        lax.fori_loop(0, count // TILE, tile, 0)

    def rank(d):
        pb, ps = peer(d)
        return pb * ns + ps

    load_angle.wait()
    load_key.wait()
    turn(me, 0, places)
    load_value.wait()
    store_value = pltpu.make_async_copy(own, ovalue_ref.at[me], local_sem.at[3])
    store_value.start()
    for i in range(max(len(near), len(far))):
        if i < len(far):
            hop(0, far[i]).wait_recv()
            forward(0, far[i]).start()
            hop(1, far[i]).start()
        if i < len(near):
            direct(0, near[i]).wait_recv()
            turn(rank(near[i]), 0, places)
    for d in far:
        direct(0, d).wait_recv()
        turn(rank(d), 0, half // heads)
        hop(1, d).wait_recv()
        forward(1, d).start()
        forward(0, d).wait_recv()
        turn(rank(d), half // heads, rest // heads)

    for h in range(heads):
        scale_ref[h:h + 1, :] = jnp.max(peak[h].T, axis=0, keepdims=True)
        inverse = 1.0 / jnp.max(peak[h], axis=1, keepdims=True)

        def narrow(i, carry):
            cols = pl.ds(pl.multiple_of(i * 4 * TILE, 4 * TILE), 4 * TILE)
            okey_ref[h, :, cols] = (turned[h, :, cols] * inverse).astype(okey_ref.dtype)
            return carry

        lax.fori_loop(0, n * places // (4 * TILE), narrow, 0)

    for d in near + far:
        direct(1, d).wait_recv()
    for d in far:
        forward(1, d).wait_recv()
    for a in range(2):
        for d in near + far:
            direct(a, d).wait_send()
        for d in far:
            hop(a, d).wait_send()
            forward(a, d).wait_send()
    store_value.wait()


def settle(keys_in, values_in, keys_out, values_out):
    keys_out[...] = keys_in[...]
    values_out[...] = values_in[...]


def body(nb, ns, ng, key_rows, value_rows, turn_angle, key_gain):
    n, places, heads, size = key_rows.shape
    rows = places * heads
    length = n * places
    rest = rows - (rows // 2) // (TILE * heads) * (TILE * heads)
    bf16, f32 = jnp.bfloat16, jnp.float32
    dma = pltpu.SemaphoreType.DMA
    whole = pl.BlockSpec(memory_space=pltpu.VMEM)
    hbm = pl.BlockSpec(memory_space=ANY)
    keys, values, scale = pl.pallas_call(
        functools.partial(exchange, nb, ns, ng, heads),
        out_shape=(
            jax.ShapeDtypeStruct((heads, size, length), bf16),
            jax.ShapeDtypeStruct((n, rows, size), bf16),
            jax.ShapeDtypeStruct((heads, size), f32),
        ),
        in_specs=[hbm, hbm, hbm, whole],
        out_specs=(whole, hbm, whole),
        scratch_shapes=[
            pltpu.VMEM((n, rows, size), bf16),
            pltpu.VMEM((2, n - ns, rest, size), bf16),
            pltpu.VMEM((heads, size, length), f32),
            pltpu.VMEM((size // 2, length), f32),
            pltpu.VMEM((size, size), f32),
            pltpu.VMEM((heads, size, TILE), f32),
            pltpu.VMEM((TILE * heads, size), f32),
            pltpu.VMEM((rows, size), bf16),
            dma((2, n)), dma((2, n)), dma((2, n)), dma((2, n)), dma((2, n)), dma((2, n)), dma((4,)),
        ],
        compiler_params=pltpu.CompilerParams(
            collective_id=0, has_side_effects=True, vmem_limit_bytes=60 * 1024 * 1024
        ),
    )(
        key_rows.reshape(n, rows, size),
        value_rows.reshape(n, rows, size),
        turn_angle.T,
        key_gain.reshape(1, size),
    )
    key_block = pl.BlockSpec((heads, size // n, length), lambda i: (0, i, 0))
    value_block = pl.BlockSpec((1, rows, size), lambda i: (i, 0, 0))
    keys, values = pl.pallas_call(
        settle,
        grid=(n,),
        out_shape=(
            jax.ShapeDtypeStruct(keys.shape, bf16),
            jax.ShapeDtypeStruct(values.shape, bf16),
        ),
        in_specs=[key_block, value_block],
        out_specs=(key_block, value_block),
    )(keys, values)
    return keys[None], values.reshape(1, length, heads, size), scale[None]


def solution(mesh):
    nb, ns, ng = (mesh.shape[a] for a in ("block", "span", "group"))
    return jax.shard_map(
        functools.partial(body, nb, ns, ng),
        mesh=mesh,
        in_specs=(
            P(None, ("block", "span"), "group", None),
            P(None, ("block", "span"), "group", None),
            P(),
            P(),
        ),
        out_specs=(
            P(("block", "span"), "group", None, None),
            P(("block", "span"), None, "group", None),
            P(("block", "span"), "group", None),
        ),
        check_vma=False,
    )
```

```python
import functools

import jax
import jax.numpy as jnp
from jax import lax
from jax.experimental import pallas as pl
from jax.experimental.pallas import tpu as pltpu
from jax.sharding import PartitionSpec as P

MESH = pl.DeviceIdType.MESH
ANY = pltpu.MemorySpace.HBM
TILE = 128
EPS = 1e-06


def flip(index, offset, size):
    out, width = 0, 1
    while width < size:
        out = out + ((index // width) % 2 + (offset // width) % 2) % 2 * width
        width *= 2
    return out


def sin_cos(angle):
    h = angle * 0.5
    q = h * h
    s = 1.0 / 6227020800.0
    for c in (-1.0 / 39916800, 1.0 / 362880, -1.0 / 5040, 1.0 / 120, -1.0 / 6, 1.0):
        s = s * q + c
    s = s * h
    k = -1.0 / 87178291200.0
    for c in (1.0 / 479001600, -1.0 / 3628800, 1.0 / 40320, -1.0 / 720, 1.0 / 24, -0.5, 1.0):
        k = k * q + c
    return 2.0 * s * k, 1.0 - 2.0 * s * s


def exchange(
    nb, ns, ng, heads,
    key_ref, value_ref, angle_ref, gain_ref,
    okey_ref, ovalue_ref, scale_ref,
    kbuf, turned, angles, gains, peak, wide,
    send_sem, recv_sem, local_sem,
):
    n, rows = key_ref.shape[0], key_ref.shape[1]
    places = rows // heads
    size = wide.shape[1]
    mid = size // 2
    b, s, g = (lax.axis_index(a) for a in ("block", "span", "group"))
    me = b * ns + s

    def peer(d):
        return (b + d // ns) % nb, flip(s, d % ns, ns)

    far = [d for d in range(ns, n)]
    near = [d for d in range(1, ns)]

    bar = pltpu.get_barrier_semaphore()
    for d in near + far:
        pb, ps = peer(d)
        pl.semaphore_signal(bar, inc=1, device_id=(pb, ps, g), device_id_type=MESH)
    pl.semaphore_wait(bar, n - 1)

    sources = (key_ref, value_ref)
    sinks = (kbuf, ovalue_ref)

    def direct(a, d):
        pb, ps = peer(d)
        r = pb * ns + ps
        return pltpu.make_async_remote_copy(
            src_ref=sources[a].at[r], dst_ref=sinks[a].at[me],
            send_sem=send_sem.at[a, d], recv_sem=recv_sem.at[a, d],
            device_id=(pb, ps, g), device_id_type=MESH,
        )

    order = []
    for i in range(max(len(near), len(far))):
        order += far[i:i + 1] + near[i:i + 1]
    for d in order:
        direct(0, d).start()
    load_angle = pltpu.make_async_copy(angle_ref, angles, local_sem.at[0])
    load_angle.start()
    load_key = pltpu.make_async_copy(key_ref.at[me], kbuf.at[me], local_sem.at[1])
    load_key.start()
    load_value = pltpu.make_async_copy(value_ref.at[me], ovalue_ref.at[me], local_sem.at[2])
    load_value.start()
    for d in order:
        direct(1, d).start()

    gains[...] = jnp.broadcast_to(gain_ref[...], (size, size)).T
    peak[...] = jnp.zeros_like(peak)

    def turn(r, first, count):
        def tile(i, carry):
            at = first + i * TILE
            wide[...] = kbuf[r, pl.ds(pl.multiple_of(at * heads, TILE * heads), TILE * heads), :].astype(jnp.float32)
            cols = pl.ds(pl.multiple_of(r * places + at, TILE), TILE)
            sine, cosine = sin_cos(angles[:, cols])
            for h in range(heads):
                x = wide[pl.ds(h, TILE, stride=heads), :].T
                norm = lax.rsqrt(jnp.mean(x * x, axis=0, keepdims=True) + EPS)
                x = x * norm * gains[...]
                lo, hi = x[:mid], x[mid:]
                lo, hi = lo * cosine - hi * sine, hi * cosine + lo * sine
                turned[h, :mid, cols] = lo
                turned[h, mid:, cols] = hi
                peak[h, :mid] = jnp.maximum(peak[h, :mid], jnp.abs(lo))
                peak[h, mid:] = jnp.maximum(peak[h, mid:], jnp.abs(hi))
            return carry

        lax.fori_loop(0, count // TILE, tile, 0)

    def rank(d):
        pb, ps = peer(d)
        return pb * ns + ps

    load_angle.wait()
    load_key.wait()
    turn(me, 0, places)
    for d in order:
        direct(0, d).wait_recv()
        turn(rank(d), 0, places)

    for h in range(heads):
        scale_ref[h:h + 1, :] = jnp.max(peak[h].T, axis=0, keepdims=True)
        inverse = 1.0 / jnp.max(peak[h], axis=1, keepdims=True)

        def narrow(i, carry):
            cols = pl.ds(pl.multiple_of(i * 4 * TILE, 4 * TILE), 4 * TILE)
            okey_ref[h, :, cols] = (turned[h, :, cols] * inverse).astype(okey_ref.dtype)
            return carry

        lax.fori_loop(0, n * places // (4 * TILE), narrow, 0)

    for d in order:
        direct(1, d).wait_recv()
    for d in order:
        direct(0, d).wait_send()
        direct(1, d).wait_send()
    load_value.wait()


def settle(keys_in, values_in, scale_in, keys_out, values_out, scale_out, sem):
    copies = [
        pltpu.make_async_copy(keys_in, keys_out, sem.at[0]),
        pltpu.make_async_copy(values_in, values_out, sem.at[1]),
        pltpu.make_async_copy(scale_in, scale_out, sem.at[2]),
    ]
    for copy in copies:
        copy.start()
    for copy in copies:
        copy.wait()


def body(nb, ns, ng, key_rows, value_rows, turn_angle, key_gain):
    n, places, heads, size = key_rows.shape
    rows = places * heads
    length = n * places
    bf16, f32 = jnp.bfloat16, jnp.float32
    dma = pltpu.SemaphoreType.DMA
    whole = pl.BlockSpec(memory_space=pltpu.VMEM)
    hbm = pl.BlockSpec(memory_space=ANY)
    keys, values, scale = pl.pallas_call(
        functools.partial(exchange, nb, ns, ng, heads),
        out_shape=(
            pltpu.VMEM((heads, size, length), bf16),
            pltpu.VMEM((n, rows, size), bf16),
            pltpu.VMEM((heads, size), f32),
        ),
        in_specs=[hbm, hbm, hbm, whole],
        out_specs=(whole, whole, whole),
        scratch_shapes=[
            pltpu.VMEM((n, rows, size), bf16),
            pltpu.VMEM((heads, size, length), f32),
            pltpu.VMEM((size // 2, length), f32),
            pltpu.VMEM((size, size), f32),
            pltpu.VMEM((heads, size, TILE), f32),
            pltpu.VMEM((TILE * heads, size), f32),
            dma((2, n)), dma((2, n)), dma((3,)),
        ],
        compiler_params=pltpu.CompilerParams(
            collective_id=0, has_side_effects=True, vmem_limit_bytes=50 * 1024 * 1024
        ),
    )(
        key_rows.reshape(n, rows, size),
        value_rows.reshape(n, rows, size),
        turn_angle.T,
        key_gain.reshape(1, size),
    )
    keys, values, scale = pl.pallas_call(
        settle,
        out_shape=(
            jax.ShapeDtypeStruct(keys.shape, bf16),
            jax.ShapeDtypeStruct(values.shape, bf16),
            jax.ShapeDtypeStruct(scale.shape, f32),
        ),
        in_specs=[whole, whole, whole],
        out_specs=(hbm, hbm, hbm),
        scratch_shapes=[dma((3,))],
        compiler_params=pltpu.CompilerParams(vmem_limit_bytes=1024 * 1024),
    )(keys, values, scale)
    return keys[None], values.reshape(1, length, heads, size), scale[None]


def solution(mesh):
    nb, ns, ng = (mesh.shape[a] for a in ("block", "span", "group"))
    return jax.shard_map(
        functools.partial(body, nb, ns, ng),
        mesh=mesh,
        in_specs=(
            P(None, ("block", "span"), "group", None),
            P(None, ("block", "span"), "group", None),
            P(),
            P(),
        ),
        out_specs=(
            P(("block", "span"), "group", None, None),
            P(("block", "span"), None, "group", None),
            P(("block", "span"), "group", None),
        ),
        check_vma=False,
    )
```
